256 devices in a mesh: pipe: 8 (over x, core), dp: 8 (over z), tensor: 4 (over y).
Axes of the slice: x: 4, y: 4, z: 8, core: 2. Of those that a mesh axis runs over, the one named last changes fastest.
Arguments:
- acts_in: bfloat16 [2, 1024, 4096], P(None, 'dp', 'tensor'), may hold values from -6 to 6
- weights: bfloat16 [8, 4096, 4096], P('pipe', None, 'tensor'), may hold values from -0.046875 to 0.046875
- cotangent: bfloat16 [2, 1024, 4096], P(None, 'dp', 'tensor'), may hold values from -6 to 6
- hist_act: float32 [8, 16], P('pipe'), may hold values from 2 to 12
- hist_weight: float32 [8, 16], P('pipe'), may hold values from 0.01 to 0.1
- hist_grad: float32 [8, 16], P('pipe'), may hold values from 2 to 12
Outputs:
- section_acts: bfloat16 [8, 2, 1024, 4096], P('pipe', None, 'dp', 'tensor')
- section_grads: bfloat16 [8, 2, 1024, 4096], P('pipe', None, 'dp', 'tensor')
- weight_grad: bfloat16 [8, 4096, 4096], P('pipe', 'dp', 'tensor')
- new_hist_act: float32 [8, 16], P('pipe')
- new_hist_weight: float32 [8, 16], P('pipe')
- new_hist_grad: float32 [8, 16], P('pipe')
The draws below stay inside these ranges and needn't reach their ends.
All inputs are finite; a program needn't handle non-finite values.
Results may differ from the reference program's by a relative error of at most 0.025.
Values may be sent and summed in bfloat16 or wider, within the bound.
No kernel may reach another device: no remote copies, remote signals or barrier semaphores. Data moves between devices by JAX's collectives and lax.ppermute only.
A program may use at most 128 MiB of HBM per device.

```python
import math
import jax
import jax.numpy as jnp
from jax import lax

D = 4096
ROWS = 128
MICRO = 2
HIST = 16
SECTIONS = 8
BATCH = 1024
N_DP = 8
N_TENSOR = 4


def steps_of(key, dims, split, least, high):
    factor_of, own = 1.0, jax.random.fold_in(key, 6)
    for axis_at, blocks in split:
        draws = jnp.exp(jax.random.uniform(jax.random.fold_in(own, axis_at), (blocks,), jnp.float32, least / len(split), high / len(split)))
        factor_of = factor_of * jnp.repeat(draws, dims[axis_at] // blocks).reshape([-1 if axis == axis_at else 1 for axis in range(len(dims))])
    return factor_of


def centred(rng, shape, scale, reach, pieces=(), kind=jnp.bfloat16):
    factor_of = steps_of(rng, shape, pieces, -0.22, 0.18) if pieces else 1.0
    result = jax.random.normal(rng, shape, jnp.float32) * scale * factor_of
    return jnp.minimum(jnp.maximum(result, -reach), reach).astype(kind)


def setup_inputs(seed: int = 0) -> dict:
    seeds = jax.random.split(jax.random.key(seed), 7)
    acts_in = centred(seeds[0], (MICRO, BATCH, D), 1.0, 6.0, ((1, 8), (2, 4)))
    weights = centred(seeds[1], (SECTIONS, D, D), (4 * D) ** -0.5, 0.046875, ((0, 8), (2, 4)))
    cotangent = centred(seeds[2], (MICRO, BATCH, D), 1.0, 6.0, ((1, 8), (2, 4)))
    hist_act = jnp.clip(jnp.exp(math.log(12.0) - 1.7917595 * jax.random.uniform(seeds[3], (SECTIONS, HIST), jnp.float32) ** steps_of(seeds[3], (SECTIONS, HIST), ((0, 8),), -0.2, 0.2)), 2.0, 12.0)
    hist_weight = jnp.clip(jnp.exp(math.log(0.1) - 2.3025851 * jax.random.uniform(seeds[4], (SECTIONS, HIST), jnp.float32) ** steps_of(seeds[4], (SECTIONS, HIST), ((0, 8),), -0.2, 0.2)), 0.01, 0.1)
    hist_grad = jnp.clip(jnp.exp(math.log(12.0) - 1.7917595 * jax.random.uniform(seeds[5], (SECTIONS, HIST), jnp.float32) ** steps_of(seeds[5], (SECTIONS, HIST), ((0, 8),), -0.2, 0.2)), 2.0, 12.0)
    return {"acts_in": acts_in, "weights": weights, "cotangent": cotangent, "hist_act": hist_act, "hist_weight": hist_weight, "hist_grad": hist_grad}


def quantize(values, factor, limit_value):
    return jnp.clip(values.astype(jnp.float32) * factor, -limit_value, limit_value).astype(jnp.bfloat16)


def settle(values):
    return lax.optimization_barrier(values.astype(jnp.bfloat16)).astype(jnp.float32)


def roll_history(history, newest):
    return jnp.concatenate([newest[:, None], history[:, :-1]], axis=1)


def reference(acts_in, weights, cotangent, hist_act, hist_weight, hist_grad):
    section_count = weights.shape[0]
    full_width = weights.shape[1]
    block_width = full_width // N_TENSOR
    current = acts_in.reshape(-1, full_width)
    act_factors = []
    weight_factors = []
    quant_acts = []
    quant_weights = []
    outputs = []
    act_peaks = []
    weight_peaks = []
    for section_index in range(section_count):
        act_factor = 448.0 / jnp.max(hist_act[section_index])
        weight_factor = 448.0 / jnp.max(hist_weight[section_index])
        quant_weight = quantize(weights[section_index], weight_factor, 448.0)
        quant_act = quantize(current, act_factor, 448.0)
        act_peaks.append(jnp.max(jnp.abs(current.astype(jnp.float32))))
        weight_peaks.append(jnp.max(jnp.abs(weights[section_index].astype(jnp.float32))))
        mixed_terms = jnp.dot(quant_act, quant_weight, preferred_element_type=jnp.float32) * (1.0 / (act_factor * weight_factor))
        current = (current.astype(jnp.float32) + mixed_terms).astype(jnp.bfloat16)
        outputs.append(current.reshape(MICRO, -1, full_width))
        act_factors.append(act_factor)
        weight_factors.append(weight_factor)
        quant_acts.append(quant_act)
        quant_weights.append(quant_weight)
    gradient = (cotangent.reshape(-1, full_width).astype(jnp.float32) * current.astype(jnp.float32)).astype(jnp.bfloat16)
    grads_out = [None] * section_count
    weight_sums = [None] * section_count
    grad_peaks = [None] * section_count
    for section_index in reversed(range(section_count)):
        grad_factor = 57344.0 / jnp.max(hist_grad[section_index])
        grad_peaks[section_index] = jnp.max(jnp.abs(gradient.astype(jnp.float32)))
        quant_grad = quantize(gradient, grad_factor, 57344.0)
        backward_factor = 1.0 / (grad_factor * weight_factors[section_index])
        sum_total = jnp.zeros((gradient.shape[0], full_width), jnp.float32)
        for shard_part in range(N_TENSOR):
            column_span = slice(shard_part * block_width, (shard_part + 1) * block_width)
            product_term = jnp.dot(quant_grad[:, column_span], quant_weights[section_index][:, column_span].T, preferred_element_type=jnp.float32) * backward_factor
            sum_total = sum_total + settle(product_term)
        gradient = (gradient.astype(jnp.float32) + sum_total).astype(jnp.bfloat16)
        grads_out[section_index] = gradient.reshape(MICRO, -1, full_width)
        update_factor = 1.0 / (act_factors[section_index] * grad_factor)
        acts_split = quant_acts[section_index].reshape(MICRO, N_DP, ROWS, full_width)
        grads_split = quant_grad.reshape(MICRO, N_DP, ROWS, full_width)
        weight_sum = jnp.zeros((full_width, full_width), jnp.float32)
        for dp_rank in range(N_DP):
            left_rows = acts_split[:, dp_rank].reshape(-1, full_width)
            right_rows = grads_split[:, dp_rank].reshape(-1, full_width)
            weight_sum = weight_sum + settle(jnp.dot(left_rows.T, right_rows, preferred_element_type=jnp.float32) * update_factor)
        weight_sums[section_index] = weight_sum.astype(jnp.bfloat16)
    section_acts = jnp.stack(outputs)
    section_grads = jnp.stack(grads_out)
    weight_grad = jnp.stack(weight_sums)
    new_hist_act = roll_history(hist_act, jnp.stack(act_peaks))
    new_hist_weight = roll_history(hist_weight, jnp.stack(weight_peaks))
    new_hist_grad = roll_history(hist_grad, jnp.stack(grad_peaks))
    return (section_acts, section_grads, weight_grad, new_hist_act, new_hist_weight, new_hist_grad)
```

```python
import jax
import jax.numpy as jnp
from jax import lax
from jax.sharding import PartitionSpec as P

AXES = ("pipe", "dp", "tensor")
CHUNKS = 4


def sent(value, stages, turn):
    sections, copies, blocks = (lax.axis_size(a) for a in AXES)

    def place(s, d, t):
        return (s % sections * copies + d) * blocks + t % blocks

    pairs = [
        (place(s, d, t), place(s + stages, d, t + turn))
        for s in range(sections)
        for d in range(copies)
        for t in range(blocks)
    ]
    return lax.ppermute(value, AXES, pairs)


def quantize(values, factor, limit_value):
    return jnp.clip(values.astype(jnp.float32) * factor, -limit_value, limit_value).astype(
        jnp.bfloat16
    )


def roll_history(history, newest):
    return jnp.concatenate([jnp.reshape(newest, (1, 1)), history[:, :-1]], axis=1)


def peak_of(values):
    return jnp.max(jnp.abs(values)).astype(jnp.float32)


def copy_for_each(array, axis):
    copies = jnp.broadcast_to(array, (lax.axis_size(axis), *array.shape))
    return lax.all_to_all(copies, axis, split_axis=0, concat_axis=0, tiled=True)


def shards(acts_in, weights, cotangent, hist_act, hist_weight, hist_grad):
    section = lax.axis_index("pipe")
    block = lax.axis_index("tensor")
    sections = lax.axis_size("pipe")
    blocks = lax.axis_size("tensor")
    width = acts_in.shape[2]
    rows = acts_in.shape[0] * acts_in.shape[1]
    chunk = rows // CHUNKS
    acts = acts_in.reshape(CHUNKS, chunk, width)
    cots = cotangent.reshape(CHUNKS, chunk, width)
    weight = weights[0]
    act_factor = 448.0 / jnp.max(hist_act)
    weight_factor = 448.0 / jnp.max(hist_weight)
    grad_factor = 57344.0 / jnp.max(hist_grad)
    forward_factor = 1.0 / (act_factor * weight_factor)
    backward_factor = 1.0 / (grad_factor * weight_factor)
    update_factor = 1.0 / (act_factor * grad_factor)
    first_column = [(block + blocks - k) % blocks * width for k in range(blocks)]

    outs = jnp.zeros((CHUNKS + 1, chunk, width), jnp.bfloat16)
    stash = jnp.zeros((CHUNKS + 1, chunk, width * blocks), jnp.bfloat16)
    held = jnp.zeros((CHUNKS + 1, chunk, width), jnp.bfloat16)
    sums = jnp.zeros((CHUNKS + 1, chunk, width), jnp.bfloat16)
    act_peak = jnp.float32(0.0)
    grad_peak = jnp.float32(0.0)

    def slot_of(index):
        live = (index >= 0) & (index < CHUNKS)
        return live, jnp.where(live, index, CHUNKS)

    arrived = [sent(acts[0], 1, k) for k in range(blocks)]
    quant_weight = [
        quantize(lax.dynamic_slice_in_dim(weight, c, width, 0), weight_factor, 448.0)
        for c in first_column
    ]
    returned = None
    output = None
    forward_ticks = CHUNKS + sections - 1
    last_tick = CHUNKS + 2 * sections - 2
    for tick in range(last_tick + 1):
        previous = output
        if tick < forward_ticks:
            live, slot = slot_of(tick - section)
            terms = jnp.zeros((chunk, width), jnp.float32)
            for k in range(blocks):
                quant = quantize(arrived[k], act_factor, 448.0)
                stash = lax.dynamic_update_slice(stash, quant[None], (slot, 0, first_column[k]))
                terms = terms + jnp.dot(
                    quant, quant_weight[k], preferred_element_type=jnp.float32
                )
            output = (arrived[0].astype(jnp.float32) + terms * forward_factor).astype(
                jnp.bfloat16
            )
            act_peak = jnp.maximum(act_peak, jnp.where(live, peak_of(arrived[0]), 0.0))
            outs = lax.dynamic_update_slice(outs, output[None], (slot, 0, 0))
            if tick + 1 < forward_ticks:
                leaving = output
                if tick + 1 < CHUNKS:
                    leaving = jnp.where(section == sections - 1, acts[tick + 1], output)
                arrived = [sent(leaving, 1, k) for k in range(blocks)]
        if tick >= sections:
            live, slot = slot_of(tick - (2 * sections - 1) + section)
            gradient = None
            if returned is not None:
                total = sum(r.astype(jnp.float32) for r in returned)
                gradient = total.astype(jnp.bfloat16)
                index = jnp.where(section == sections - 1, tick - 2 * sections, tick - (2 * sections - 1) + section)
                sums = lax.dynamic_update_slice(sums, gradient[None], (slot_of(index)[1], 0, 0))
            if tick < sections + CHUNKS:
                first = (
                    cots[tick - sections].astype(jnp.float32) * previous.astype(jnp.float32)
                ).astype(jnp.bfloat16)
                gradient = (
                    first
                    if gradient is None
                    else jnp.where(section == sections - 1, first, gradient)
                )
            quant = quantize(gradient, grad_factor, 57344.0)
            held = lax.dynamic_update_slice(held, quant[None], (slot, 0, 0))
            grad_peak = jnp.maximum(grad_peak, jnp.where(live, peak_of(gradient), 0.0))
            returned = []
            for k in range(blocks):
                part = (
                    lax.dot_general(
                        quant,
                        quant_weight[-k % blocks],
                        (((1,), (1,)), ((), ())),
                        preferred_element_type=jnp.float32,
                    )
                    * backward_factor
                )
                if k == 0:
                    part = part + gradient.astype(jnp.float32)
                returned.append(
                    sent(part.astype(jnp.bfloat16), 0 if tick == last_tick else -1, k)
                )
    last = sum(r.astype(jnp.float32) for r in returned).astype(jnp.bfloat16)
    grads = sent(sums[:CHUNKS], 1, 0)
    grads = jnp.concatenate(
        [grads[: CHUNKS - 1], jnp.where(section == 0, last, grads[CHUNKS - 1])[None]]
    )
    weight_peak = peak_of(weight)
    weight_sums = lax.psum_scatter(
        (
            lax.dot_general(
                stash[:CHUNKS].reshape(rows, width * blocks),
                held[:CHUNKS].reshape(rows, width),
                (((0,), (0,)), ((), ())),
                preferred_element_type=jnp.float32,
            )
            * update_factor
        ).astype(jnp.bfloat16),
        "dp",
        scatter_dimension=0,
        tiled=True,
    )
    peaks = copy_for_each(jnp.stack([act_peak, weight_peak, grad_peak]), ("dp", "tensor")).max(axis=0)
    return (
        outs[:CHUNKS].reshape(1, *acts_in.shape),
        grads.reshape(1, *acts_in.shape),
        weight_sums[None],
        roll_history(hist_act, peaks[0]),
        roll_history(hist_weight, peaks[1]),
        roll_history(hist_grad, peaks[2]),
    )


def solution(mesh):
    rows = P(None, "dp", "tensor")
    saved = P("pipe", None, "dp", "tensor")
    history = P("pipe", None)
    return jax.shard_map(
        shards,
        mesh=mesh,
        in_specs=(rows, P("pipe", None, "tensor"), rows, history, history, history),
        out_specs=(saved, saved, P("pipe", "dp", "tensor"), history, history, history),
        check_vma=False,
    )
```

```python
import jax
import jax.numpy as jnp
from jax import lax
from jax.sharding import PartitionSpec as P

AXES = ("pipe", "dp", "tensor")
CHUNKS = 4


def sent(value, stages, turn, copy=0):
    sections, copies, blocks = (lax.axis_size(a) for a in AXES)

    def place(s, d, t):
        return (s % sections * copies + d % copies) * blocks + t % blocks

    pairs = [
        (place(s, d, t), place(s + stages, d + copy, t + turn))
        for s in range(sections)
        for d in range(copies)
        for t in range(blocks)
    ]
    return lax.ppermute(value, AXES, pairs)


def quantize(values, factor, limit_value):
    return jnp.clip(values.astype(jnp.float32) * factor, -limit_value, limit_value).astype(
        jnp.bfloat16
    )


def roll_history(history, newest):
    return jnp.concatenate([jnp.reshape(newest, (1, 1)), history[:, :-1]], axis=1)


def shards(acts_in, weights, cotangent, hist_act, hist_weight, hist_grad):
    section = lax.axis_index("pipe")
    block = lax.axis_index("tensor")
    sections = lax.axis_size("pipe")
    blocks = lax.axis_size("tensor")
    width = acts_in.shape[2]
    rows = acts_in.shape[0] * acts_in.shape[1]
    chunk = rows // CHUNKS
    acts = acts_in.reshape(CHUNKS, chunk, width)
    cots = cotangent.reshape(CHUNKS, chunk, width)
    weight = weights[0]
    act_factor = 448.0 / jnp.max(hist_act)
    weight_factor = 448.0 / jnp.max(hist_weight)
    grad_factor = 57344.0 / jnp.max(hist_grad)
    forward_factor = 1.0 / (act_factor * weight_factor)
    backward_factor = 1.0 / (grad_factor * weight_factor)
    update_factor = 1.0 / (act_factor * grad_factor)
    first_column = [(block + blocks - k) % blocks * width for k in range(blocks)]

    outs = jnp.zeros((CHUNKS + 1, chunk, width), jnp.bfloat16)
    copies = lax.axis_size("dp")
    share = width * blocks // copies
    per_block = width // share
    stash = jnp.zeros((copies, (CHUNKS + 1) * chunk, share), jnp.bfloat16)
    held = jnp.zeros((CHUNKS + 1, chunk, width), jnp.bfloat16)
    sums = jnp.zeros((CHUNKS + 1, chunk, width), jnp.bfloat16)
    act_sizes = jnp.zeros((chunk, width), jnp.bfloat16)
    grad_sizes = jnp.zeros((chunk, width), jnp.bfloat16)

    def slot_of(index):
        live = (index >= 0) & (index < CHUNKS)
        return live, jnp.where(live, index, CHUNKS)

    arrived = [sent(acts[0], 1, k) for k in range(blocks)]
    quant_weight = [
        quantize(lax.dynamic_slice_in_dim(weight, c, width, 0), weight_factor, 448.0)
        for c in first_column
    ]
    quant_weight = lax.optimization_barrier(quant_weight)
    returned = None
    output = None
    forward_ticks = CHUNKS + sections - 1
    last_tick = CHUNKS + 2 * sections - 2
    for tick in range(last_tick + 1):
        previous = output
        if tick < forward_ticks:
            live, slot = slot_of(tick - section)
            terms = jnp.zeros((chunk, width), jnp.float32)
            for k in range(blocks):
                quant = quantize(arrived[k], act_factor, 448.0)
                stash = lax.dynamic_update_slice(
                    stash,
                    quant.reshape(chunk, per_block, share).swapaxes(0, 1),
                    (first_column[k] // share, slot * chunk, 0),
                )
                terms = terms + jnp.dot(
                    quant, quant_weight[k], preferred_element_type=jnp.float32
                )
            output = (arrived[0].astype(jnp.float32) + terms * forward_factor).astype(
                jnp.bfloat16
            )
            act_sizes = jnp.where(live, jnp.maximum(act_sizes, jnp.abs(arrived[0])), act_sizes)
            outs = lax.dynamic_update_slice(outs, output[None], (slot, 0, 0))
            if tick == forward_ticks - 1:
                quant_acts = lax.all_to_all(
                    stash[:, : CHUNKS * chunk], "dp", split_axis=0, concat_axis=0, tiled=True
                )
            if tick + 1 < forward_ticks:
                leaving = output
                if tick + 1 < CHUNKS:
                    leaving = jnp.where(section == sections - 1, acts[tick + 1], output)
                arrived = [sent(leaving, 1, k) for k in range(blocks)]
        if tick >= sections:
            live, slot = slot_of(tick - (2 * sections - 1) + section)
            gradient = None
            if returned is not None:
                total = sum(r.astype(jnp.float32) for r in returned)
                gradient = total.astype(jnp.bfloat16)
                index = jnp.where(section == sections - 1, tick - 2 * sections, tick - (2 * sections - 1) + section)
                sums = lax.dynamic_update_slice(sums, gradient[None], (slot_of(index)[1], 0, 0))
            if tick < sections + CHUNKS:
                first = (
                    cots[tick - sections].astype(jnp.float32) * previous.astype(jnp.float32)
                ).astype(jnp.bfloat16)
                gradient = (
                    first
                    if gradient is None
                    else jnp.where(section == sections - 1, first, gradient)
                )
            quant = quantize(gradient, grad_factor, 57344.0)
            held = lax.dynamic_update_slice(held, quant[None], (slot, 0, 0))
            grad_sizes = jnp.where(live, jnp.maximum(grad_sizes, jnp.abs(gradient)), grad_sizes)
            if tick == last_tick - 1:
                early = lax.all_gather(
                    held[: CHUNKS - 1].reshape(-1, width), "dp", axis=0, tiled=False
                )
            returned = []
            for k in range(blocks):
                part = (
                    lax.dot_general(
                        quant,
                        quant_weight[-k % blocks],
                        (((1,), (1,)), ((), ())),
                        preferred_element_type=jnp.float32,
                    )
                    * backward_factor
                )
                if k == 0:
                    part = part + gradient.astype(jnp.float32)
                part = part.astype(jnp.bfloat16)
                if tick < last_tick:
                    part = sent(part, -1, k)
                elif k > 0:
                    part = sent(part, 0, k)
                returned.append(part)
    last = sum(r.astype(jnp.float32) for r in returned).astype(jnp.bfloat16)
    grads = sent(sums[:CHUNKS], 1, 0)
    grads = jnp.concatenate(
        [grads[: CHUNKS - 1], jnp.where(section == 0, last, grads[CHUNKS - 1])[None]]
    )
    peaks = jnp.stack([jnp.max(act_sizes), jnp.max(jnp.abs(weight)), jnp.max(grad_sizes)])
    lanes = lax.broadcasted_iota(jnp.int32, (16, width), 0)
    notes = jnp.where(lanes == 0, peaks[0], jnp.where(lanes == 1, peaks[1], peaks[2]))
    piece = jnp.concatenate([held[CHUNKS - 1], notes])
    pieces = [piece]
    owners = [0]
    for direction, steps in ((1, copies // 2), (-1, copies - 1 - copies // 2)):
        moving = piece
        for step in range(steps):
            moving = sent(moving, 0, 0, direction)
            pieces.append(moving)
            owners.append(-direction * (step + 1))
    place = lax.axis_index("dp")
    late_rows = slice((CHUNKS - 1) * chunk, CHUNKS * chunk)
    late_acts = jnp.concatenate(
        [
            lax.dynamic_index_in_dim(
                quant_acts[:, late_rows], (place + o + copies) % copies, 0, keepdims=False
            )
            for o in owners
        ]
    )
    late_grads = jnp.concatenate([p[:chunk] for p in pieces])
    rows_first = (((0,), (0,)), ((), ()))
    weight_grad = lax.dot_general(
        late_acts, late_grads, rows_first, preferred_element_type=jnp.float32
    ) + lax.dot_general(
        quant_acts[:, : late_rows.start].reshape(-1, share),
        early.reshape(-1, width),
        rows_first,
        preferred_element_type=jnp.float32,
    )
    weight_grad = (weight_grad * update_factor).astype(jnp.bfloat16)
    largest = jnp.stack([p[chunk:, :128] for p in pieces]).max(axis=0)
    for turn in (1, 2):
        largest = jnp.maximum(largest, sent(largest, 0, turn))
    peaks = largest[:3, 0].astype(jnp.float32)
    return (
        outs[:CHUNKS].reshape(1, *acts_in.shape),
        grads.reshape(1, *acts_in.shape),
        weight_grad[None],
        roll_history(hist_act, peaks[0]),
        roll_history(hist_weight, peaks[1]),
        roll_history(hist_grad, peaks[2]),
    )


def solution(mesh):
    rows = P(None, "dp", "tensor")
    saved = P("pipe", None, "dp", "tensor")
    history = P("pipe", None)
    return jax.shard_map(
        shards,
        mesh=mesh,
        in_specs=(rows, P("pipe", None, "tensor"), rows, history, history, history),
        out_specs=(saved, saved, P("pipe", "dp", "tensor"), history, history, history),
        check_vma=False,
    )
```

```python
import jax
import jax.numpy as jnp
from jax import lax
from jax.sharding import PartitionSpec as P


AXES = ("pipe", "dp", "tensor")
CHUNKS = 4
EARLY = 2
TURNS = (2, 1, 3, 0)


def sent(value, stages, turn, copy=0):
    sections, copies, blocks = (lax.axis_size(a) for a in AXES)

    def place(s, d, t):
        return (s % sections * copies + d % copies) * blocks + t % blocks

    pairs = [
        (place(s, d, t), place(s + stages, d + copy, t + turn))
        for s in range(sections)
        for d in range(copies)
        for t in range(blocks)
    ]
    return lax.ppermute(value, AXES, pairs)


def quantize(values, factor, limit_value):
    return jnp.clip(values.astype(jnp.float32) * factor, -limit_value, limit_value).astype(
        jnp.bfloat16
    )


def roll_history(history, newest):
    return jnp.concatenate([jnp.reshape(newest, (1, 1)), history[:, :-1]], axis=1)


def shards(acts_in, weights, cotangent, hist_act, hist_weight, hist_grad):
    section = lax.axis_index("pipe")
    block = lax.axis_index("tensor")
    sections = lax.axis_size("pipe")
    blocks = lax.axis_size("tensor")
    width = acts_in.shape[2]
    rows = acts_in.shape[0] * acts_in.shape[1]
    chunk = rows // CHUNKS
    acts = acts_in.reshape(CHUNKS, chunk, width)
    cots = cotangent.reshape(CHUNKS, chunk, width)
    weight = weights[0]
    largest = jnp.max(jnp.concatenate([hist_act, hist_weight, hist_grad]), axis=1)
    act_factor = 448.0 / largest[0]
    weight_factor = 448.0 / largest[1]
    grad_factor = 57344.0 / largest[2]
    forward_factor = 1.0 / (act_factor * weight_factor)
    backward_factor = 1.0 / (grad_factor * weight_factor)
    update_factor = 1.0 / (act_factor * grad_factor)
    first_column = [(block + blocks - k) % blocks * width for k in range(blocks)]

    outs = jnp.zeros((CHUNKS + 1, chunk, width), jnp.bfloat16)
    copies = lax.axis_size("dp")
    share = width * blocks // copies
    per_block = width // share
    stash = jnp.zeros((copies, (CHUNKS + 1) * chunk, share), jnp.bfloat16)
    held = jnp.zeros((CHUNKS + 1, chunk, width), jnp.bfloat16)
    sums = jnp.zeros((CHUNKS + 1, chunk, width), jnp.bfloat16)
    act_sizes = jnp.zeros((chunk, width), jnp.bfloat16)
    grad_sizes = jnp.zeros((chunk, width), jnp.bfloat16)

    def slot_of(index):
        live = (index >= 0) & (index < CHUNKS)
        return live, jnp.where(live, index, CHUNKS)

    arrived = [sent(acts[0], 1, k) for k in range(blocks)]
    quant_weight = [
        quantize(lax.dynamic_slice_in_dim(weight, c, width, 0), weight_factor, 448.0)
        for c in first_column
    ]
    quant_weight = lax.optimization_barrier(quant_weight)
    weight_sizes = []
    returned = None
    output = None
    forward_ticks = CHUNKS + sections - 1
    last_tick = CHUNKS + 2 * sections - 2
    for tick in range(last_tick + 1):
        previous = output
        if tick < forward_ticks:
            live, slot = slot_of(tick - section)
            terms = jnp.zeros((chunk, width), jnp.float32)
            for k in (TURNS[1], TURNS[0], *TURNS[2:]):
                quant = quantize(arrived[k], act_factor, 448.0)
                stash = lax.dynamic_update_slice(
                    stash,
                    quant.reshape(chunk, per_block, share).swapaxes(0, 1),
                    (first_column[k] // share, slot * chunk, 0),
                )
                terms = terms + jnp.dot(
                    quant, quant_weight[k], preferred_element_type=jnp.float32
                )
            output = (arrived[0].astype(jnp.float32) + terms * forward_factor).astype(
                jnp.bfloat16
            )
            act_sizes = jnp.where(live, jnp.maximum(act_sizes, jnp.abs(arrived[0])), act_sizes)
            outs = lax.dynamic_update_slice(outs, output[None], (slot, 0, 0))
            if tick == forward_ticks - 1:
                quant_acts = lax.all_to_all(
                    stash[:, : CHUNKS * chunk], "dp", split_axis=0, concat_axis=0, tiled=True
                )
            if tick + 1 < forward_ticks:
                leaving = output
                if tick + 1 < CHUNKS:
                    leaving = jnp.where(section == sections - 1, acts[tick + 1], output)
                arrived = [None] * blocks
                if 0 < tick <= blocks:
                    weight, leaving = lax.optimization_barrier((weight, leaving))
                    part = lax.slice_in_dim(weight, (tick - 1) * width, tick * width)
                    weight_sizes.append(jnp.max(jnp.abs(part)))
                for k in TURNS:
                    arrived[k] = sent(leaving, 1, k)
        if tick >= sections:
            live, slot = slot_of(tick - (2 * sections - 1) + section)
            gradient = None
            if returned is not None:
                total = sum(r.astype(jnp.float32) for r in returned)
                gradient = total.astype(jnp.bfloat16)
                index = jnp.where(section == sections - 1, tick - 2 * sections, tick - (2 * sections - 1) + section)
                sums = lax.dynamic_update_slice(sums, gradient[None], (slot_of(index)[1], 0, 0))
            if tick < sections + CHUNKS:
                first = (
                    cots[tick - sections].astype(jnp.float32) * previous.astype(jnp.float32)
                ).astype(jnp.bfloat16)
                gradient = (
                    first
                    if gradient is None
                    else jnp.where(section == sections - 1, first, gradient)
                )
            quant = quantize(gradient, grad_factor, 57344.0)
            held = lax.dynamic_update_slice(held, quant[None], (slot, 0, 0))
            grad_sizes = jnp.where(live, jnp.maximum(grad_sizes, jnp.abs(gradient)), grad_sizes)
            if tick == last_tick - CHUNKS + EARLY:
                early = lax.all_gather(
                    held[:EARLY].reshape(-1, width), "dp", axis=0, tiled=False
                )
            returned = []
            for k in TURNS:
                part = (
                    lax.dot_general(
                        quant,
                        quant_weight[-k % blocks],
                        (((1,), (1,)), ((), ())),
                        preferred_element_type=jnp.float32,
                    )
                    * backward_factor
                )
                if k == 0:
                    part = part + gradient.astype(jnp.float32)
                part = part.astype(jnp.bfloat16)
                if tick < last_tick:
                    part = sent(part, -1, k)
                elif k > 0:
                    part = sent(part, 0, k)
                returned.append(part)
    last = sum(r.astype(jnp.float32) for r in returned).astype(jnp.bfloat16)
    grads = sent(sums[:CHUNKS], 1, 0)
    grads = jnp.concatenate(
        [grads[: CHUNKS - 1], jnp.where(section == 0, last, grads[CHUNKS - 1])[None]]
    )
    peaks = jnp.stack([jnp.max(act_sizes), jnp.stack(weight_sizes).max(), jnp.max(grad_sizes)])
    peaks = jnp.broadcast_to(peaks[:, None], (3, 128))
    for turn, copy in ((1, 0), (2, 0), (0, 1), (0, 2), (0, 4)):
        others = sent(peaks, 0, turn, copy)
        peaks = jnp.maximum(peaks, others)
    peaks = peaks[:, 0].astype(jnp.float32)
    place = lax.axis_index("dp")
    rows_first = (((0,), (0,)), ((), ()))

    def late_product(piece, owner):
        owner_acts = lax.dynamic_slice(
            quant_acts,
            ((place + owner + copies) % copies, EARLY * chunk, 0),
            (1, (CHUNKS - EARLY) * chunk, share),
        )[0]
        return lax.dot_general(owner_acts, piece, rows_first, preferred_element_type=jnp.float32)

    piece = held[EARLY:CHUNKS].reshape(-1, width)
    weight_grad = late_product(piece, 0)
    up = down = piece
    for step in range(1, copies // 2 + 1):
        up = sent(up, 0, 0, 1)
        if step < copies // 2:
            down = sent(down, 0, 0, -1)
        if step == copies // 2 - 1:
            weight_grad = weight_grad + lax.dot_general(
                quant_acts[:, : EARLY * chunk].reshape(-1, share),
                early.reshape(-1, width),
                rows_first,
                preferred_element_type=jnp.float32,
            )
        weight_grad = weight_grad + late_product(up, -step)
        if step < copies // 2:
            weight_grad = weight_grad + late_product(down, step)
    weight_grad = (weight_grad * update_factor).astype(jnp.bfloat16)
    return (
        outs[:CHUNKS].reshape(1, *acts_in.shape),
        grads.reshape(1, *acts_in.shape),
        weight_grad[None],
        roll_history(hist_act, peaks[0]),
        roll_history(hist_weight, peaks[1]),
        roll_history(hist_grad, peaks[2]),
    )


def solution(mesh):
    rows = P(None, "dp", "tensor")
    saved = P("pipe", None, "dp", "tensor")
    history = P("pipe", None)
    return jax.shard_map(
        shards,
        mesh=mesh,
        in_specs=(rows, P("pipe", None, "tensor"), rows, history, history, history),
        out_specs=(saved, saved, P("pipe", "dp", "tensor"), history, history, history),
        check_vma=False,
    )
```

```python
import jax
import jax.numpy as jnp
from jax import lax
from jax.experimental.layout import Layout, with_layout_constraint
from jax.sharding import PartitionSpec as P


AXES = ("pipe", "dp", "tensor")
CHUNKS = 4
EARLY = 2
TURNS = (2, 1, 3, 0)


def sent(value, stages, turn, copy=0):
    sections, copies, blocks = (lax.axis_size(a) for a in AXES)

    def place(s, d, t):
        return (s % sections * copies + d % copies) * blocks + t % blocks

    pairs = [
        (place(s, d, t), place(s + stages, d + copy, t + turn))
        for s in range(sections)
        for d in range(copies)
        for t in range(blocks)
    ]
    return lax.ppermute(value, AXES, pairs)


def quantize(values, factor, limit_value):
    return jnp.clip(values.astype(jnp.float32) * factor, -limit_value, limit_value).astype(
        jnp.bfloat16
    )


def roll_history(history, newest):
    return jnp.concatenate([jnp.reshape(newest, (1, 1)), history[:, :-1]], axis=1)


def row_major(array):
    return with_layout_constraint(array, Layout(major_to_minor=tuple(range(array.ndim))))


def shards(acts_in, weights, cotangent, hist_act, hist_weight, hist_grad):
    section = lax.axis_index("pipe")
    block = lax.axis_index("tensor")
    sections = lax.axis_size("pipe")
    blocks = lax.axis_size("tensor")
    width = acts_in.shape[2]
    rows = acts_in.shape[0] * acts_in.shape[1]
    chunk = rows // CHUNKS
    acts = acts_in.reshape(CHUNKS, chunk, width)
    cots = cotangent.reshape(CHUNKS, chunk, width)
    weight = weights[0]
    largest = jnp.max(jnp.concatenate([hist_act, hist_weight, hist_grad]), axis=1)
    act_factor = 448.0 / largest[0]
    weight_factor = 448.0 / largest[1]
    grad_factor = 57344.0 / largest[2]
    forward_factor = 1.0 / (act_factor * weight_factor)
    backward_factor = 1.0 / (grad_factor * weight_factor)
    update_factor = 1.0 / (act_factor * grad_factor)
    first_column = [(block + blocks - k) % blocks * width for k in range(blocks)]

    outs = jnp.zeros((CHUNKS + 1, chunk, width), jnp.bfloat16)
    copies = lax.axis_size("dp")
    share = width * blocks // copies
    per_block = width // share
    stash = jnp.zeros((copies, (CHUNKS + 1) * chunk, share), jnp.bfloat16)
    held = jnp.zeros((CHUNKS + 1, chunk, width), jnp.bfloat16)
    sums = jnp.zeros((CHUNKS + 1, chunk, width), jnp.bfloat16)
    act_sizes = jnp.zeros((chunk, width), jnp.bfloat16)
    grad_sizes = jnp.zeros((chunk, width), jnp.bfloat16)

    def slot_of(index):
        live = (index >= 0) & (index < CHUNKS)
        return live, jnp.where(live, index, CHUNKS)

    arrived = [sent(acts[0], 1, k) for k in range(blocks)]
    quant_weight = [
        quantize(lax.dynamic_slice_in_dim(weight, c, width, 0), weight_factor, 448.0)
        for c in first_column
    ]
    quant_weight = lax.optimization_barrier(quant_weight)
    weight_sizes = []
    returned = None
    output = None
    forward_ticks = CHUNKS + sections - 1
    last_tick = CHUNKS + 2 * sections - 2
    for tick in range(last_tick + 1):
        previous = output
        if tick < forward_ticks:
            live, slot = slot_of(tick - section)
            terms = jnp.zeros((chunk, width), jnp.float32)
            for k in (TURNS[1], TURNS[0], *TURNS[2:]):
                quant = quantize(arrived[k], act_factor, 448.0)
                stash = lax.dynamic_update_slice(
                    stash,
                    quant.reshape(chunk, per_block, share).swapaxes(0, 1),
                    (first_column[k] // share, slot * chunk, 0),
                )
                terms = terms + jnp.dot(
                    quant, quant_weight[k], preferred_element_type=jnp.float32
                )
            output = (arrived[0].astype(jnp.float32) + terms * forward_factor).astype(
                jnp.bfloat16
            )
            act_sizes = jnp.where(live, jnp.maximum(act_sizes, jnp.abs(arrived[0])), act_sizes)
            outs = lax.dynamic_update_slice(outs, output[None], (slot, 0, 0))
            if tick == forward_ticks - 1:
                leaving_acts = row_major(stash[:, : CHUNKS * chunk])
                quant_acts = lax.all_to_all(
                    leaving_acts, "dp", split_axis=0, concat_axis=0, tiled=True
                )
                quant_acts = row_major(quant_acts)
            if tick + 1 < forward_ticks:
                leaving = output
                if tick + 1 < CHUNKS:
                    leaving = jnp.where(section == sections - 1, acts[tick + 1], output)
                arrived = [None] * blocks
                if 0 < tick <= blocks:
                    weight, leaving = lax.optimization_barrier((weight, leaving))
                    part = lax.slice_in_dim(weight, (tick - 1) * width, tick * width)
                    weight_sizes.append(jnp.max(jnp.abs(part)))
                for k in TURNS:
                    arrived[k] = sent(leaving, 1, k)
        if tick >= sections:
            live, slot = slot_of(tick - (2 * sections - 1) + section)
            gradient = None
            if returned is not None:
                total = sum(r.astype(jnp.float32) for r in returned)
                gradient = total.astype(jnp.bfloat16)
                index = jnp.where(section == sections - 1, tick - 2 * sections, tick - (2 * sections - 1) + section)
                sums = lax.dynamic_update_slice(sums, gradient[None], (slot_of(index)[1], 0, 0))
            if tick < sections + CHUNKS:
                first = (
                    cots[tick - sections].astype(jnp.float32) * previous.astype(jnp.float32)
                ).astype(jnp.bfloat16)
                gradient = (
                    first
                    if gradient is None
                    else jnp.where(section == sections - 1, first, gradient)
                )
            quant = quantize(gradient, grad_factor, 57344.0)
            held = lax.dynamic_update_slice(held, quant[None], (slot, 0, 0))
            grad_sizes = jnp.where(live, jnp.maximum(grad_sizes, jnp.abs(gradient)), grad_sizes)
            if tick == last_tick - CHUNKS + EARLY:
                early = lax.all_gather(
                    held[:EARLY].reshape(-1, width), "dp", axis=0, tiled=False
                )
            returned = []
            for k in TURNS:
                part = (
                    lax.dot_general(
                        quant,
                        quant_weight[-k % blocks],
                        (((1,), (1,)), ((), ())),
                        preferred_element_type=jnp.float32,
                    )
                    * backward_factor
                )
                if k == 0:
                    part = part + gradient.astype(jnp.float32)
                part = part.astype(jnp.bfloat16)
                if tick < last_tick:
                    part = sent(part, -1, k)
                elif k > 0:
                    part = sent(part, 0, k)
                returned.append(part)
    last = sum(r.astype(jnp.float32) for r in returned).astype(jnp.bfloat16)
    grads = sent(sums[:CHUNKS], 1, 0)
    grads = jnp.concatenate(
        [grads[: CHUNKS - 1], jnp.where(section == 0, last, grads[CHUNKS - 1])[None]]
    )
    peaks = jnp.stack([jnp.max(act_sizes), jnp.stack(weight_sizes).max(), jnp.max(grad_sizes)])
    peaks = jnp.broadcast_to(peaks[:, None], (3, 128))
    for turn, copy in ((1, 0), (2, 0), (0, 1), (0, 2), (0, 4)):
        others = sent(peaks, 0, turn, copy)
        peaks = jnp.maximum(peaks, others)
    peaks = peaks[:, 0].astype(jnp.float32)
    early_rows = EARLY * chunk
    piece = held[EARLY:CHUNKS].reshape(-1, width)
    up = [piece]
    down = []
    for step in range(1, copies // 2 + 1):
        up.append(sent(up[-1], 0, 0, 1))
        if step < copies // 2:
            down.append(sent(down[-1] if down else piece, 0, 0, -1))
    late_acts = jnp.concatenate([quant_acts[:, early_rows:]] * 2)
    first = (lax.axis_index("dp") + copies - copies // 2) % copies
    late_acts = lax.dynamic_slice_in_dim(late_acts, first, copies)
    late_acts = row_major(lax.optimization_barrier(late_acts))
    rows_first = (((0,), (0,)), ((), ()))
    weight_grad = lax.dot_general(
        quant_acts[:, :early_rows].reshape(-1, share),
        early.reshape(-1, width),
        rows_first,
        preferred_element_type=jnp.float32,
    )
    late_grads = jnp.concatenate(up[::-1] + down)
    weight_grad = weight_grad + lax.dot_general(
        late_acts.reshape(-1, share), late_grads, rows_first, preferred_element_type=jnp.float32
    )
    weight_grad = (weight_grad * update_factor).astype(jnp.bfloat16)
    return (
        outs[:CHUNKS].reshape(1, *acts_in.shape),
        grads.reshape(1, *acts_in.shape),
        weight_grad[None],
        roll_history(hist_act, peaks[0]),
        roll_history(hist_weight, peaks[1]),
        roll_history(hist_grad, peaks[2]),
    )


def solution(mesh):
    rows = P(None, "dp", "tensor")
    saved = P("pipe", None, "dp", "tensor")
    history = P("pipe", None)
    return jax.shard_map(
        shards,
        mesh=mesh,
        in_specs=(rows, P("pipe", None, "tensor"), rows, history, history, history),
        out_specs=(saved, saved, P("pipe", "dp", "tensor"), history, history, history),
        check_vma=False,
    )
```

```python
import jax
import jax.numpy as jnp
from jax import lax
from jax.experimental.layout import Layout, with_layout_constraint
from jax.sharding import PartitionSpec as P


AXES = ("pipe", "dp", "tensor")
CHUNKS = 4
EARLY = 2
TURNS = (2, 1, 3, 0)


def sent(value, stages, turn, copy=0):
    sections, copies, blocks = (lax.axis_size(a) for a in AXES)

    def place(s, d, t):
        return (s % sections * copies + d % copies) * blocks + t % blocks

    pairs = [
        (place(s, d, t), place(s + stages, d + copy, t + turn))
        for s in range(sections)
        for d in range(copies)
        for t in range(blocks)
    ]
    return lax.ppermute(value, AXES, pairs)


class Ring:
    def __init__(self, rows):
        self.up = [rows]
        self.down = [rows]

    def turn(self):
        half = lax.axis_size("dp") // 2
        step = len(self.up)
        self.up.append(sent(self.up[-1], 0, 0, 1))
        if step < half:
            self.down.append(sent(self.down[-1], 0, 0, -1))

    def laid_out(self):
        return jnp.concatenate(self.up[::-1] + self.down[1:])


def quantize(values, factor, limit_value):
    return jnp.clip(values.astype(jnp.float32) * factor, -limit_value, limit_value).astype(
        jnp.bfloat16
    )


def roll_history(history, newest):
    return jnp.concatenate([jnp.reshape(newest, (1, 1)), history[:, :-1]], axis=1)


def row_major(array):
    return with_layout_constraint(array, Layout(major_to_minor=tuple(range(array.ndim))))


def shards(acts_in, weights, cotangent, hist_act, hist_weight, hist_grad):
    section = lax.axis_index("pipe")
    block = lax.axis_index("tensor")
    sections = lax.axis_size("pipe")
    blocks = lax.axis_size("tensor")
    width = acts_in.shape[2]
    rows = acts_in.shape[0] * acts_in.shape[1]
    chunk = rows // CHUNKS
    acts = acts_in.reshape(CHUNKS, chunk, width)
    cots = cotangent.reshape(CHUNKS, chunk, width)
    weight = weights[0]
    largest = jnp.max(jnp.concatenate([hist_act, hist_weight, hist_grad]), axis=1)
    act_factor = 448.0 / largest[0]
    weight_factor = 448.0 / largest[1]
    grad_factor = 57344.0 / largest[2]
    forward_factor = 1.0 / (act_factor * weight_factor)
    backward_factor = 1.0 / (grad_factor * weight_factor)
    update_factor = 1.0 / (act_factor * grad_factor)
    first_column = [(block + blocks - k) % blocks * width for k in range(blocks)]

    outs = jnp.zeros((CHUNKS + 1, chunk, width), jnp.bfloat16)
    copies = lax.axis_size("dp")
    share = width * blocks // copies
    per_block = width // share
    stash = jnp.zeros((copies, (CHUNKS + 1) * chunk, share), jnp.bfloat16)
    held = jnp.zeros((CHUNKS + 1, chunk, width), jnp.bfloat16)
    sums = jnp.zeros((CHUNKS + 1, chunk, width), jnp.bfloat16)
    act_sizes = jnp.zeros((chunk, width), jnp.bfloat16)
    grad_sizes = jnp.zeros((chunk, width), jnp.bfloat16)

    def slot_of(index):
        live = (index >= 0) & (index < CHUNKS)
        return live, jnp.where(live, index, CHUNKS)

    arrived = [sent(acts[0], 1, k) for k in range(blocks)]
    quant_weight = [
        quantize(lax.dynamic_slice_in_dim(weight, c, width, 0), weight_factor, 448.0)
        for c in first_column
    ]
    quant_weight = lax.optimization_barrier(quant_weight)
    weight_sizes = []
    returned = None
    output = None
    forward_ticks = CHUNKS + sections - 1
    last_tick = CHUNKS + 2 * sections - 2
    for tick in range(last_tick + 1):
        previous = output
        if tick < forward_ticks:
            live, slot = slot_of(tick - section)
            terms = jnp.zeros((chunk, width), jnp.float32)
            for k in (TURNS[1], TURNS[0], *TURNS[2:]):
                quant = quantize(arrived[k], act_factor, 448.0)
                stash = lax.dynamic_update_slice(
                    stash,
                    quant.reshape(chunk, per_block, share).swapaxes(0, 1),
                    (first_column[k] // share, slot * chunk, 0),
                )
                terms = terms + jnp.dot(
                    quant, quant_weight[k], preferred_element_type=jnp.float32
                )
            output = (arrived[0].astype(jnp.float32) + terms * forward_factor).astype(
                jnp.bfloat16
            )
            act_sizes = jnp.where(live, jnp.maximum(act_sizes, jnp.abs(arrived[0])), act_sizes)
            outs = lax.dynamic_update_slice(outs, output[None], (slot, 0, 0))
            if tick == forward_ticks - 1:
                leaving_acts = row_major(stash)
                quant_acts = lax.all_to_all(
                    leaving_acts, "dp", split_axis=0, concat_axis=0, tiled=True
                )
                quant_acts = row_major(quant_acts)
            if tick + 1 < forward_ticks:
                leaving = output
                if tick + 1 < CHUNKS:
                    leaving = jnp.where(section == sections - 1, acts[tick + 1], output)
                arrived = [None] * blocks
                if 0 < tick <= blocks:
                    weight, leaving = lax.optimization_barrier((weight, leaving))
                    part = lax.slice_in_dim(weight, (tick - 1) * width, tick * width)
                    weight_sizes.append(jnp.max(jnp.abs(part)))
                for k in TURNS:
                    arrived[k] = sent(leaving, 1, k)
        if tick >= sections:
            live, slot = slot_of(tick - (2 * sections - 1) + section)
            gradient = None
            if returned is not None:
                total = sum(r.astype(jnp.float32) for r in returned)
                gradient = total.astype(jnp.bfloat16)
                index = jnp.where(section == sections - 1, tick - 2 * sections, tick - (2 * sections - 1) + section)
                sums = lax.dynamic_update_slice(sums, gradient[None], (slot_of(index)[1], 0, 0))
            if tick < sections + CHUNKS:
                first = (
                    cots[tick - sections].astype(jnp.float32) * previous.astype(jnp.float32)
                ).astype(jnp.bfloat16)
                gradient = (
                    first
                    if gradient is None
                    else jnp.where(section == sections - 1, first, gradient)
                )
            quant = quantize(gradient, grad_factor, 57344.0)
            held = lax.dynamic_update_slice(held, quant[None], (slot, 0, 0))
            grad_sizes = jnp.where(live, jnp.maximum(grad_sizes, jnp.abs(gradient)), grad_sizes)
            if tick == last_tick - CHUNKS + EARLY:
                first_ring = Ring(held[:EARLY].reshape(-1, width))
                first_ring.turn()
                first_ring.turn()
            if tick == last_tick - 1:
                first_ring.turn()
            if tick == last_tick:
                second_ring = Ring(held[EARLY:CHUNKS].reshape(-1, width))
                second_ring.turn()
                first_ring.turn()
                for _ in range(3):
                    second_ring.turn()
            returned = []
            for k in TURNS:
                part = (
                    lax.dot_general(
                        quant,
                        quant_weight[-k % blocks],
                        (((1,), (1,)), ((), ())),
                        preferred_element_type=jnp.float32,
                    )
                    * backward_factor
                )
                if k == 0:
                    part = part + gradient.astype(jnp.float32)
                part = part.astype(jnp.bfloat16)
                if tick < last_tick:
                    part = sent(part, -1, k)
                elif k > 0:
                    part = sent(part, 0, k)
                returned.append(part)
    last = sum(r.astype(jnp.float32) for r in returned).astype(jnp.bfloat16)
    grads = sent(sums[:CHUNKS], 1, 0)
    grads = jnp.concatenate(
        [grads[: CHUNKS - 1], jnp.where(section == 0, last, grads[CHUNKS - 1])[None]]
    )
    peaks = jnp.stack([jnp.max(act_sizes), jnp.stack(weight_sizes).max(), jnp.max(grad_sizes)])
    peaks = jnp.broadcast_to(peaks[:, None], (3, 128))
    for turn, copy in ((1, 0), (2, 0), (0, 1), (0, 2), (0, 4)):
        others = sent(peaks, 0, turn, copy)
        peaks = jnp.maximum(peaks, others)
    peaks = peaks[:, 0].astype(jnp.float32)
    own_acts = jnp.concatenate([quant_acts[:, : CHUNKS * chunk]] * 2)
    first = (lax.axis_index("dp") + copies - copies // 2) % copies
    own_acts = lax.dynamic_slice_in_dim(own_acts, first, copies)
    own_acts = row_major(lax.optimization_barrier(own_acts))
    rows_first = (((0,), (0,)), ((), ()))
    early_acts = own_acts[:, : EARLY * chunk]
    late_acts = own_acts[:, EARLY * chunk :]
    near = slice(1, copies - 1)

    def product(acts, grads):
        return lax.dot_general(
            acts.reshape(-1, share), grads, rows_first, preferred_element_type=jnp.float32
        )

    weight_grad = product(early_acts, first_ring.laid_out())
    near_grads = jnp.concatenate(second_ring.up[-2::-1] + second_ring.down[1:-1])
    weight_grad = weight_grad + product(late_acts[near], near_grads)
    far_grads = jnp.concatenate([second_ring.up[-1], second_ring.down[-1]])
    far_acts = jnp.concatenate([late_acts[:1], late_acts[-1:]])
    weight_grad = weight_grad + product(far_acts, far_grads)
    weight_grad = (weight_grad * update_factor).astype(jnp.bfloat16)
    return (
        outs[:CHUNKS].reshape(1, *acts_in.shape),
        grads.reshape(1, *acts_in.shape),
        weight_grad[None],
        roll_history(hist_act, peaks[0]),
        roll_history(hist_weight, peaks[1]),
        roll_history(hist_grad, peaks[2]),
    )


def solution(mesh):
    rows = P(None, "dp", "tensor")
    saved = P("pipe", None, "dp", "tensor")
    history = P("pipe", None)
    return jax.shard_map(
        shards,
        mesh=mesh,
        in_specs=(rows, P("pipe", None, "tensor"), rows, history, history, history),
        out_specs=(saved, saved, P("pipe", "dp", "tensor"), history, history, history),
        check_vma=False,
    )
```

```python
import jax
import jax.numpy as jnp
from jax import lax
from jax.experimental.layout import Layout, with_layout_constraint
from jax.sharding import PartitionSpec as P


AXES = ("pipe", "dp", "tensor")
CHUNKS = 4
EARLY = 2
TURNS = (2, 1, 3, 0)


def sent(value, stages, turn, copy=0):
    sections, copies, blocks = (lax.axis_size(a) for a in AXES)

    def place(s, d, t):
        return (s % sections * copies + d % copies) * blocks + t % blocks

    pairs = [
        (place(s, d, t), place(s + stages, d + copy, t + turn))
        for s in range(sections)
        for d in range(copies)
        for t in range(blocks)
    ]
    return lax.ppermute(value, AXES, pairs)


class Ring:
    def __init__(self, rows):
        self.up = [rows]
        self.down = [rows]

    def turn(self):
        half = lax.axis_size("dp") // 2
        step = len(self.up)
        self.up.append(sent(self.up[-1], 0, 0, 1))
        if step < half:
            self.down.append(sent(self.down[-1], 0, 0, -1))


def quantize(values, factor, limit_value):
    return jnp.clip(values.astype(jnp.float32) * factor, -limit_value, limit_value).astype(
        jnp.bfloat16
    )


def roll_history(history, newest):
    return jnp.concatenate([jnp.reshape(newest, (1, 1)), history[:, :-1]], axis=1)


def row_major(array):
    return with_layout_constraint(array, Layout(major_to_minor=tuple(range(array.ndim))))


def shards(acts_in, weights, cotangent, hist_act, hist_weight, hist_grad):
    section = lax.axis_index("pipe")
    block = lax.axis_index("tensor")
    sections = lax.axis_size("pipe")
    blocks = lax.axis_size("tensor")
    width = acts_in.shape[2]
    rows = acts_in.shape[0] * acts_in.shape[1]
    chunk = rows // CHUNKS
    acts = acts_in.reshape(CHUNKS, chunk, width)
    cots = cotangent.reshape(CHUNKS, chunk, width)
    weight = weights[0]
    largest = jnp.max(jnp.concatenate([hist_act, hist_weight, hist_grad]), axis=1)
    act_factor = 448.0 / largest[0]
    weight_factor = 448.0 / largest[1]
    grad_factor = 57344.0 / largest[2]
    forward_factor = 1.0 / (act_factor * weight_factor)
    backward_factor = 1.0 / (grad_factor * weight_factor)
    update_factor = 1.0 / (act_factor * grad_factor)
    first_column = [(block + blocks - k) % blocks * width for k in range(blocks)]

    outs = jnp.zeros((CHUNKS + 1, chunk, width), jnp.bfloat16)
    copies = lax.axis_size("dp")
    share = width * blocks // copies
    per_block = width // share
    stash = jnp.zeros((copies, (CHUNKS + 1) * chunk, share), jnp.bfloat16)
    held = jnp.zeros((CHUNKS + 1, chunk, width), jnp.bfloat16)
    sums = jnp.zeros((CHUNKS + 1, chunk, width), jnp.bfloat16)
    act_sizes = jnp.zeros((chunk, width), jnp.bfloat16)
    grad_sizes = jnp.zeros((chunk, width), jnp.bfloat16)

    def slot_of(index):
        live = (index >= 0) & (index < CHUNKS)
        return live, jnp.where(live, index, CHUNKS)

    arrived = [sent(acts[0], 1, k) for k in range(blocks)]
    quant_weight = [
        quantize(lax.dynamic_slice_in_dim(weight, c, width, 0), weight_factor, 448.0)
        for c in first_column
    ]
    quant_weight = lax.optimization_barrier(quant_weight)
    weight_sizes = []
    returned = None
    output = None
    forward_ticks = CHUNKS + sections - 1
    last_tick = CHUNKS + 2 * sections - 2
    for tick in range(last_tick + 1):
        previous = output
        if tick < forward_ticks:
            live, slot = slot_of(tick - section)
            terms = jnp.zeros((chunk, width), jnp.float32)
            for k in (TURNS[1], TURNS[0], *TURNS[2:]):
                quant = quantize(arrived[k], act_factor, 448.0)
                stash = lax.dynamic_update_slice(
                    stash,
                    quant.reshape(chunk, per_block, share).swapaxes(0, 1),
                    (first_column[k] // share, slot * chunk, 0),
                )
                terms = terms + jnp.dot(
                    quant, quant_weight[k], preferred_element_type=jnp.float32
                )
            output = (arrived[0].astype(jnp.float32) + terms * forward_factor).astype(
                jnp.bfloat16
            )
            act_sizes = jnp.where(live, jnp.maximum(act_sizes, jnp.abs(arrived[0])), act_sizes)
            outs = lax.dynamic_update_slice(outs, output[None], (slot, 0, 0))
            if tick == forward_ticks - 1:
                leaving_acts = row_major(stash)
                quant_acts = lax.all_to_all(
                    leaving_acts, "dp", split_axis=0, concat_axis=0, tiled=True
                )
                quant_acts = row_major(quant_acts)
            if tick + 1 < forward_ticks:
                leaving = output
                if tick + 1 < CHUNKS:
                    leaving = jnp.where(section == sections - 1, acts[tick + 1], output)
                arrived = [None] * blocks
                if 0 < tick <= blocks:
                    weight, leaving = lax.optimization_barrier((weight, leaving))
                    part = lax.slice_in_dim(weight, (tick - 1) * width, tick * width)
                    weight_sizes.append(jnp.max(jnp.abs(part)))
                for k in TURNS:
                    arrived[k] = sent(leaving, 1, k)
        if tick >= sections:
            live, slot = slot_of(tick - (2 * sections - 1) + section)
            gradient = None
            if returned is not None:
                total = sum(r.astype(jnp.float32) for r in returned)
                gradient = total.astype(jnp.bfloat16)
                index = jnp.where(section == sections - 1, tick - 2 * sections, tick - (2 * sections - 1) + section)
                sums = lax.dynamic_update_slice(sums, gradient[None], (slot_of(index)[1], 0, 0))
            if tick < sections + CHUNKS:
                first = (
                    cots[tick - sections].astype(jnp.float32) * previous.astype(jnp.float32)
                ).astype(jnp.bfloat16)
                gradient = (
                    first
                    if gradient is None
                    else jnp.where(section == sections - 1, first, gradient)
                )
            quant = quantize(gradient, grad_factor, 57344.0)
            held = lax.dynamic_update_slice(held, quant[None], (slot, 0, 0))
            grad_sizes = jnp.where(live, jnp.maximum(grad_sizes, jnp.abs(gradient)), grad_sizes)
            if tick == last_tick - CHUNKS + EARLY:
                first_ring = Ring(held[:EARLY].reshape(-1, width))
                first_ring.turn()
                first_ring.turn()
            if tick == last_tick - 1:
                first_ring.turn()
            if tick == last_tick:
                second_ring = Ring(held[EARLY:CHUNKS].reshape(-1, width))
                second_ring.turn()
                first_ring.turn()
                for _ in range(3):
                    second_ring.turn()
            returned = []
            for k in TURNS:
                part = (
                    lax.dot_general(
                        quant,
                        quant_weight[-k % blocks],
                        (((1,), (1,)), ((), ())),
                        preferred_element_type=jnp.float32,
                    )
                    * backward_factor
                )
                if k == 0:
                    part = part + gradient.astype(jnp.float32)
                part = part.astype(jnp.bfloat16)
                if tick < last_tick:
                    part = sent(part, -1, k)
                elif k > 0:
                    part = sent(part, 0, k)
                returned.append(part)
    last = sum(r.astype(jnp.float32) for r in returned).astype(jnp.bfloat16)
    grads = sent(sums[:CHUNKS], 1, 0)
    grads = jnp.concatenate(
        [grads[: CHUNKS - 1], jnp.where(section == 0, last, grads[CHUNKS - 1])[None]]
    )
    grad_size = jnp.max(grad_sizes)
    peaks = jnp.stack([jnp.max(act_sizes), jnp.stack(weight_sizes).max(), grad_size])
    peaks = jnp.broadcast_to(peaks[:, None], (3, 128))
    for turn, copy in ((1, 0), (2, 0), (0, 1), (0, 2), (0, 4)):
        others = sent(peaks, 0, turn, copy)
        peaks = jnp.maximum(peaks, others)
    peaks = peaks[:, 0].astype(jnp.float32)
    own_acts = jnp.concatenate([quant_acts[:, : CHUNKS * chunk]] * 2)
    first = (lax.axis_index("dp") + copies - copies // 2) % copies
    own_acts = lax.dynamic_slice_in_dim(own_acts, first, copies)
    own_acts = row_major(lax.optimization_barrier(own_acts))
    rows_first = (((0,), (0,)), ((), ()))
    early_acts = own_acts[:, : EARLY * chunk]
    late_acts = own_acts[:, EARLY * chunk :]
    near = slice(1, copies - 1)

    def product(acts, grads):
        return lax.dot_general(
            acts.reshape(-1, share), grads, rows_first, preferred_element_type=jnp.float32
        )

    early_grads, second_ring.up[2] = lax.optimization_barrier(
        (first_ring.up[::-1] + first_ring.down[1:], second_ring.up[2])
    )
    weight_grad = product(early_acts, jnp.concatenate(early_grads))
    near_grads = jnp.concatenate(second_ring.up[-2::-1] + second_ring.down[1:-1])
    weight_grad = weight_grad + product(late_acts[near], near_grads)
    far_grads = jnp.concatenate([second_ring.up[-1], second_ring.down[-1]])
    far_acts = jnp.concatenate([late_acts[:1], late_acts[-1:]])
    weight_grad = weight_grad + product(far_acts, far_grads)
    weight_grad = (weight_grad * update_factor).astype(jnp.bfloat16)
    return (
        outs[:CHUNKS].reshape(1, *acts_in.shape),
        grads.reshape(1, *acts_in.shape),
        weight_grad[None],
        roll_history(hist_act, peaks[0]),
        roll_history(hist_weight, peaks[1]),
        roll_history(hist_grad, peaks[2]),
    )


def solution(mesh):
    rows = P(None, "dp", "tensor")
    saved = P("pipe", None, "dp", "tensor")
    history = P("pipe", None)
    return jax.shard_map(
        shards,
        mesh=mesh,
        in_specs=(rows, P("pipe", None, "tensor"), rows, history, history, history),
        out_specs=(saved, saved, P("pipe", "dp", "tensor"), history, history, history),
        check_vma=False,
    )
```
